8 devices in a mesh: fsdp: 2 (over z, y), ep: 4 (over x, core).
Axes of the slice: x: 2, y: 2, z: 1, core: 2. Of those that a mesh axis runs over, the one named last changes fastest.
Arguments:
- x_tok: bfloat16 [32768, 1024], P(('fsdp', 'ep'))
- dy_tok: bfloat16 [32768, 1024], P(('fsdp', 'ep'))
- expert_idx: int32 [32768, 6], P(('fsdp', 'ep'))
- gate_val: float32 [32768, 6], P(('fsdp', 'ep'))
- w_one: bfloat16 [64, 1024, 704], P('ep', 'fsdp')
- w_two: bfloat16 [64, 704, 1024], P('ep', None, 'fsdp')
- w_three: bfloat16 [64, 1024, 704], P('ep', 'fsdp')
- ws_one: bfloat16 [1024, 1408], P('fsdp')
- ws_two: bfloat16 [1408, 1024], P(None, 'fsdp')
- ws_three: bfloat16 [1024, 1408], P('fsdp')
Outputs:
- output 1: bfloat16 [32768, 1024], P(('fsdp', 'ep'))
- output 2: float32 [32768, 6], P(('fsdp', 'ep'))
- output 3: float32 [64, 1024, 704], P('ep', 'fsdp')
- output 4: float32 [64, 704, 1024], P('ep', None, 'fsdp')
- output 5: float32 [64, 1024, 704], P('ep', 'fsdp')
- output 6: float32 [1024, 1408], P('fsdp')
- output 7: float32 [1408, 1024], P(None, 'fsdp')
- output 8: float32 [1024, 1408], P('fsdp')
All inputs are finite; a program needn't handle non-finite values.
Results may differ from the reference program's by a relative error of at most 0.00527379.
Values are sent between devices in bfloat16 or wider.
A program may use at most 1 GiB of HBM per device.

```python
import jax
import jax.numpy as jnp
from jax import lax

MODEL_DIM = 1024
EXPERT_FF = 704
SHARED_FF = 1408
EXPERTS = 64
TOP_K = 6
TOK_DEV = 4096
SRC_DEVICES = 8
CAPACITY = 480

TOKENS = TOK_DEV * SRC_DEVICES


def draw_routing(key):
    key_list = jax.random.split(key, 5)
    spread = EXPERTS // TOP_K
    jitter = max(spread // 4, 1)
    hot_span = max(EXPERTS // 8, 1)
    hot_start = jax.random.randint(key_list[0], (), 0, EXPERTS)
    is_hot = jax.random.randint(key_list[1], (TOKENS, 1), 0, 4) == 0
    base_hot = hot_start + jax.random.randint(key_list[2], (TOKENS, 1), 0, hot_span)
    base_any = jax.random.randint(key_list[3], (TOKENS, 1), 0, EXPERTS)
    base_id = jnp.where(is_hot, base_hot, base_any)
    offsets = jnp.arange(TOP_K, dtype=jnp.int32)[None, :] * spread + jax.random.randint(key_list[4], (TOKENS, TOP_K), 0, jitter)
    return ((base_id + offsets) % EXPERTS).astype(jnp.int32)


def setup_inputs(seed: int = 0) -> dict:
    key_list = jax.random.split(jax.random.key(seed), 10)
    dim_scale = MODEL_DIM ** -0.5
    ff_scale = EXPERT_FF ** -0.5
    shared_scale = SHARED_FF ** -0.5
    x_tok = jax.random.normal(key_list[0], (TOKENS, MODEL_DIM), jnp.float32).astype(jnp.bfloat16)
    dy_tok = jax.random.normal(key_list[1], (TOKENS, MODEL_DIM), jnp.float32).astype(jnp.bfloat16)
    expert_idx = draw_routing(key_list[2])
    gate_val = jax.random.uniform(key_list[3], (TOKENS, TOP_K), jnp.float32, 0.3, 1.0)
    w_one = (jax.random.normal(key_list[4], (EXPERTS, MODEL_DIM, EXPERT_FF), jnp.float32) * dim_scale).astype(jnp.bfloat16)
    w_two = (jax.random.normal(key_list[5], (EXPERTS, EXPERT_FF, MODEL_DIM), jnp.float32) * ff_scale).astype(jnp.bfloat16)
    w_three = (jax.random.normal(key_list[6], (EXPERTS, MODEL_DIM, EXPERT_FF), jnp.float32) * dim_scale).astype(jnp.bfloat16)
    ws_one = (jax.random.normal(key_list[7], (MODEL_DIM, SHARED_FF), jnp.float32) * dim_scale).astype(jnp.bfloat16)
    ws_two = (jax.random.normal(key_list[8], (SHARED_FF, MODEL_DIM), jnp.float32) * shared_scale).astype(jnp.bfloat16)
    ws_three = (jax.random.normal(key_list[9], (MODEL_DIM, SHARED_FF), jnp.float32) * dim_scale).astype(jnp.bfloat16)
    return {"x_tok": x_tok, "dy_tok": dy_tok, "expert_idx": expert_idx, "gate_val": gate_val, "w_one": w_one, "w_two": w_two, "w_three": w_three, "ws_one": ws_one, "ws_two": ws_two, "ws_three": ws_three}


def slots_for_source(ids_src):
    flat_ids = ids_src.reshape(-1)
    onehot = (flat_ids[:, None] == jnp.arange(EXPERTS, dtype=jnp.int32)[None, :]).astype(jnp.int32)
    slot_pos = jnp.sum(jnp.cumsum(onehot, axis=0) * onehot, axis=1) - 1
    return jnp.where(slot_pos < CAPACITY, flat_ids * CAPACITY + slot_pos, EXPERTS * CAPACITY)


def fill_for_source(slot_idx):
    n_assign = TOK_DEV * TOP_K
    filled = jnp.full((EXPERTS * CAPACITY + 1,), n_assign, jnp.int32)
    filled = filled.at[slot_idx].set(jnp.arange(n_assign, dtype=jnp.int32))
    return filled[: EXPERTS * CAPACITY]


def swiglu_grads(x_rows, g_rows, w_a, w_b, w_c):
    h_one = jnp.dot(x_rows, w_a, preferred_element_type=jnp.float32)
    h_three = jnp.dot(x_rows, w_c, preferred_element_type=jnp.float32)
    sig_one = jax.nn.sigmoid(h_one)
    silu_one = h_one * sig_one
    act_rows = (silu_one * h_three).astype(jnp.bfloat16)
    d_act = jnp.dot(g_rows, w_b.T, preferred_element_type=jnp.float32)
    dh_one = (d_act * h_three * sig_one * (1.0 + h_one * (1.0 - sig_one))).astype(jnp.bfloat16)
    dh_three = (d_act * silu_one).astype(jnp.bfloat16)
    dx_rows = (jnp.dot(dh_one, w_a.T, preferred_element_type=jnp.float32) + jnp.dot(dh_three, w_c.T, preferred_element_type=jnp.float32)).astype(jnp.bfloat16)
    dw_a = jnp.dot(x_rows.T, dh_one, preferred_element_type=jnp.float32)
    dw_b = jnp.dot(act_rows.T, g_rows, preferred_element_type=jnp.float32)
    dw_c = jnp.dot(x_rows.T, dh_three, preferred_element_type=jnp.float32)
    return dx_rows, act_rows, dw_a, dw_b, dw_c


def reference(x_tok, dy_tok, expert_idx, gate_val, w_one, w_two, w_three, ws_one, ws_two, ws_three):
    n_assign = TOK_DEV * TOP_K
    slot_idx = jax.vmap(slots_for_source)(expert_idx.reshape(SRC_DEVICES, TOK_DEV, TOP_K))
    filled = jax.vmap(fill_for_source)(slot_idx)
    src_base = jnp.arange(SRC_DEVICES, dtype=jnp.int32)[:, None] * n_assign
    global_ids = jnp.where(filled < n_assign, filled + src_base, TOKENS * TOP_K)
    expert_rows = global_ids.reshape(SRC_DEVICES, EXPERTS, CAPACITY).transpose(1, 0, 2).reshape(EXPERTS, SRC_DEVICES * CAPACITY)
    zero_row = jnp.zeros((1, MODEL_DIM), jnp.bfloat16)
    x_pad = jnp.concatenate([x_tok, zero_row])
    dy_pad = jnp.concatenate([dy_tok, zero_row])
    gate_pad = jnp.concatenate([gate_val.reshape(-1), jnp.zeros((1,), jnp.float32)])

    def expert_step(acc_state, step_in):
        dx_acc, dgate_acc = acc_state
        assign_ids, w_a, w_b, w_c = step_in
        tok_ids = assign_ids // TOP_K
        x_rows = x_pad[tok_ids]
        dy_rows = dy_pad[tok_ids]
        dy_wide = dy_rows.astype(jnp.float32)
        g_rows = (gate_pad[assign_ids][:, None] * dy_wide).astype(jnp.bfloat16)
        dx_rows, act_rows, dw_a, dw_b, dw_c = swiglu_grads(x_rows, g_rows, w_a, w_b, w_c)
        y_rows = jnp.dot(act_rows, w_b, preferred_element_type=jnp.float32)
        dgate_rows = jnp.sum(dy_wide * y_rows, axis=1)
        dx_acc = dx_acc.at[tok_ids].add(dx_rows.astype(jnp.float32))
        dgate_acc = dgate_acc.at[assign_ids].add(dgate_rows)
        return (dx_acc, dgate_acc), (dw_a, dw_b, dw_c)

    init_state = (jnp.zeros((TOKENS + 1, MODEL_DIM), jnp.float32), jnp.zeros((TOKENS * TOP_K + 1,), jnp.float32))
    final_state, expert_grads = lax.scan(expert_step, init_state, (expert_rows, w_one, w_two, w_three))

    def shared_step(acc_state, step_in):
        x_rows, dy_rows = step_in
        dx_rows, act_rows, dw_a, dw_b, dw_c = swiglu_grads(x_rows, dy_rows, ws_one, ws_two, ws_three)
        return (acc_state[0] + dw_a, acc_state[1] + dw_b, acc_state[2] + dw_c), dx_rows

    shared_init = (jnp.zeros((MODEL_DIM, SHARED_FF), jnp.float32), jnp.zeros((SHARED_FF, MODEL_DIM), jnp.float32), jnp.zeros((MODEL_DIM, SHARED_FF), jnp.float32))
    x_blocks = x_tok.reshape(SRC_DEVICES, TOK_DEV, MODEL_DIM)
    dy_blocks = dy_tok.reshape(SRC_DEVICES, TOK_DEV, MODEL_DIM)
    shared_grads, dx_shared = lax.scan(shared_step, shared_init, (x_blocks, dy_blocks))
    dx_acc, dgate_acc = final_state
    dx_out = (dx_acc[:TOKENS] + dx_shared.reshape(TOKENS, MODEL_DIM).astype(jnp.float32)).astype(jnp.bfloat16)
    dgate = dgate_acc[: TOKENS * TOP_K].reshape(TOKENS, TOP_K)
    return (dx_out, dgate, expert_grads[0], expert_grads[1], expert_grads[2], shared_grads[0], shared_grads[1], shared_grads[2])
```

```python
import jax
import jax.numpy as jnp
from jax import lax
from jax.experimental import pallas as pl
from jax.experimental.pallas import tpu as pltpu
from jax.sharding import PartitionSpec as P

CAP_NUM = 5
CAP_DEN = 4
LANES = 128
UNROLL = 8
CHUNKS = 4


def capacity_for(tok_dev, top_k, n_exp):
    needed = -(-(tok_dev * top_k * CAP_NUM) // (CAP_DEN * n_exp))
    return max(8, -(-needed // 8) * 8)


def route_slots(ids_dev, gate_dev, n_exp, capacity):
    top_k = ids_dev.shape[1]
    flat_ids = ids_dev.reshape(-1)
    n_assign = flat_ids.shape[0]
    onehot = (flat_ids[:, None] == jnp.arange(n_exp, dtype=jnp.int32)[None, :]).astype(jnp.int32)
    slot_pos = jnp.sum(jnp.cumsum(onehot, axis=0) * onehot, axis=1) - 1
    slot_idx = jnp.where(slot_pos < capacity, flat_ids * capacity + slot_pos, n_exp * capacity)
    tokens = jnp.zeros((n_exp * capacity + 1,), jnp.int32).at[slot_idx].set(jnp.arange(n_assign, dtype=jnp.int32) // top_k)
    gates = jnp.zeros((n_exp * capacity + 1,), jnp.float32).at[slot_idx].set(gate_dev.reshape(-1))
    return slot_idx, tokens[: n_exp * capacity], gates[: n_exp * capacity]


def gather_rows(tables, tokens, n_local, capacity):
    n_src = len(tables)
    tok_dev, dim = tables[0].shape
    parts = dim // LANES

    def body(tok_ref, *refs):
        tabs, out_ref, raw, wide, rows, sem = refs[:n_src], *refs[n_src:]
        src = pl.program_id(0)
        expert = pl.program_id(1)

        @pl.when(expert == 0)
        def _():
            for m in range(n_src):
                @pl.when(src == m)
                def _():
                    copy = pltpu.make_async_copy(tabs[m], raw, sem)
                    copy.start()
                    copy.wait()

            @pl.loop(0, tok_dev // LANES)
            def _(i):
                base = pl.multiple_of(i * LANES, LANES)
                for j in range(parts):
                    piece = raw[pl.ds(base, LANES), j * LANES : (j + 1) * LANES].astype(jnp.float32)
                    wide[pl.ds(base * parts + j, LANES, stride=parts), :] = piece

        first = expert * capacity

        @pl.loop(0, capacity // UNROLL)
        def _(i):
            for k in range(UNROLL):
                slot = i * UNROLL + k
                tok = pl.multiple_of(tok_ref[0, 0, first + slot] * parts, parts)
                rows[pl.ds(pl.multiple_of(slot * parts, parts), parts), :] = wide[pl.ds(tok, parts), :]

        for j in range(parts):
            out_ref[0, 0, :, j * LANES : (j + 1) * LANES] = rows[pl.ds(j, capacity, stride=parts), :].astype(out_ref.dtype)

    return pl.pallas_call(
        body,
        grid=(n_src, n_local),
        in_specs=[pl.BlockSpec((1, 1, n_local * capacity), lambda s, e: (s, 0, 0), memory_space=pltpu.SMEM)]
        + [pl.BlockSpec(memory_space=pl.ANY)] * n_src,
        out_specs=pl.BlockSpec((1, 1, capacity, dim), lambda s, e: (e, s, 0, 0)),
        out_shape=jax.ShapeDtypeStruct((n_local, n_src, capacity, dim), tables[0].dtype),
        scratch_shapes=[
            pltpu.VMEM((tok_dev, dim), tables[0].dtype),
            pltpu.VMEM((tok_dev * parts, LANES), jnp.float32),
            pltpu.VMEM((capacity * parts, LANES), jnp.float32),
            pltpu.SemaphoreType.DMA,
        ],
        compiler_params=pltpu.CompilerParams(vmem_limit_bytes=40 * 2**20),
        cost_estimate=pl.CostEstimate(flops=600_000_000, bytes_accessed=100_000_000, transcendentals=0),
        name="gather_rows",
    )(tokens.reshape(n_src, 1, n_local * capacity), *tables)


def sum_rows(row_chunks, tokens, tok_dev):
    n_chunks = len(row_chunks)
    per_chunk, n_src, capacity, dim = row_chunks[0].shape
    n_local = per_chunk * n_chunks
    parts = dim // LANES

    def body(tok_ref, *refs):
        chunks, out_ref, wide = refs[:n_chunks], *refs[n_chunks:]
        step = pl.program_id(1)

        @pl.when(step == 0)
        def _():
            @pl.loop(0, tok_dev * parts // 256)
            def _(i):
                out_ref[0, pl.ds(pl.multiple_of(i * 256, 256), 256), :] = jnp.zeros((256, LANES), jnp.float32)

        for c in range(n_chunks):
            for j in range(parts):
                wide[pl.ds(j, capacity, stride=parts), :] = chunks[c][0, 0, :, j * LANES : (j + 1) * LANES].astype(jnp.float32)
            first = (step + c * per_chunk) * capacity

            @pl.loop(0, capacity // UNROLL)
            def _(i):
                where, sums = [], []
                for k in range(UNROLL):
                    slot = i * UNROLL + k
                    tok = pl.multiple_of(tok_ref[0, 0, first + slot] * parts, parts)
                    where.append(tok)
                    row = wide[pl.ds(pl.multiple_of(slot * parts, parts), parts), :]
                    sums.append(out_ref[0, pl.ds(tok, parts), :] + row)
                for k in reversed(range(UNROLL)):
                    out_ref[0, pl.ds(where[k], parts), :] = sums[k]

    return pl.pallas_call(
        body,
        grid=(n_src, per_chunk),
        in_specs=[pl.BlockSpec((1, 1, n_local * capacity), lambda s, e: (s, 0, 0), memory_space=pltpu.SMEM)]
        + [pl.BlockSpec((1, 1, capacity, dim), lambda s, e: (e, s, 0, 0))] * n_chunks,
        out_specs=pl.BlockSpec((1, tok_dev * parts, LANES), lambda s, e: (s, 0, 0)),
        out_shape=jax.ShapeDtypeStruct((n_src, tok_dev * parts, LANES), jnp.float32),
        scratch_shapes=[pltpu.VMEM((capacity * parts, LANES), jnp.float32)],
        compiler_params=pltpu.CompilerParams(vmem_limit_bytes=56 * 2**20),
        cost_estimate=pl.CostEstimate(flops=600_000_000, bytes_accessed=130_000_000, transcendentals=0),
        name="sum_rows",
    )(tokens.reshape(n_src, 1, n_local * capacity), *row_chunks)


def swiglu_hidden(h_one, h_three, d_act):
    sig_one = jax.nn.sigmoid(h_one)
    silu_one = h_one * sig_one
    return silu_one * h_three, d_act * h_three * sig_one * (1.0 + h_one * (1.0 - sig_one)), d_act * silu_one


def dot32(form, a, b):
    return jnp.einsum(form, a, b, preferred_element_type=jnp.float32)


def solution(mesh):
    ep_size = mesh.shape["ep"]
    fs_size = mesh.shape["fsdp"]
    tok_spec = P(("fsdp", "ep"), None)
    in_specs = (tok_spec, tok_spec, tok_spec, tok_spec, P("ep", "fsdp", None), P("ep", None, "fsdp"), P("ep", "fsdp", None), P("fsdp", None), P(None, "fsdp"), P("fsdp", None))
    out_specs = (tok_spec, tok_spec, P("ep", "fsdp", None), P("ep", None, "fsdp"), P("ep", "fsdp", None), P("fsdp", None), P(None, "fsdp"), P("fsdp", None))

    def swap(value, bit):
        return lax.ppermute(value, "ep", [(i, i ^ bit) for i in range(ep_size)])

    def swap_fs(value):
        return lax.ppermute(value, "fsdp", [(i, i ^ 1) for i in range(fs_size)])

    def device_step(x_loc, dy_loc, ids_loc, gate_loc, w_one, w_two, w_three, ws_one, ws_two, ws_three):
        tok_dev, top_k = ids_loc.shape
        model_dim = x_loc.shape[1]
        n_local, _, ff = w_one.shape
        n_exp = n_local * ep_size
        capacity = capacity_for(tok_dev, top_k, n_exp)
        me = lax.axis_index("ep")
        row = lax.axis_index("fsdp")
        pick = lambda a, i, axis=0: lax.dynamic_index_in_dim(a, i, axis, keepdims=False)

        def spread(value):
            across = swap(value, 2)
            return [value, swap(value, 1), across, swap(across, 1)]

        x_tabs = spread(x_loc)
        dy_tabs = spread(dy_loc)

        slot_idx, slot_tok, slot_gate = route_slots(ids_loc, gate_loc, n_exp, capacity)
        table = jnp.stack([slot_tok.astype(jnp.float32), slot_gate]).reshape(2, ep_size, n_local, capacity).swapaxes(0, 1)
        table = lax.all_to_all(table, "ep", 0, 0, tiled=True)
        table = jnp.stack([pick(table, me ^ m) for m in range(ep_size)])
        tokens = table[:, 0].astype(jnp.int32)
        gates = table[:, 1].swapaxes(0, 1).reshape(n_local, ep_size * capacity, 1)

        per = n_local // CHUNKS
        weights = []
        for c in range(CHUNKS):
            part = slice(c * per, (c + 1) * per)
            weights.append((
                lax.all_gather(w_one[part], "fsdp", axis=1, tiled=True),
                lax.all_gather(w_three[part], "fsdp", axis=1, tiled=True),
                lax.all_gather(w_two[part], "fsdp", axis=2, tiled=True),
            ))
        ws_one_full = lax.all_gather(ws_one, "fsdp", axis=0, tiled=True)
        ws_three_full = lax.all_gather(ws_three, "fsdp", axis=0, tiled=True)
        ws_two_full = lax.all_gather(ws_two, "fsdp", axis=1, tiled=True)

        x_rows = gather_rows(x_tabs, tokens, n_local, capacity).reshape(n_local, ep_size * capacity, model_dim)
        dy_rows = gather_rows(dy_tabs, tokens, n_local, capacity).reshape(n_local, ep_size * capacity, model_dim)

        dx_chunks, dgate_chunks, grads = [], [], []
        for c in range(CHUNKS):
            part = slice(c * per, (c + 1) * per)
            w_a, w_c, w_b = weights[c]
            x_c, gate_c = x_rows[part], gates[part]
            dy_c = dy_rows[part].astype(jnp.float32)
            g_c = (gate_c * dy_c).astype(jnp.bfloat16)
            h_one = dot32("erd,edf->erf", x_c, w_a)
            h_three = dot32("erd,edf->erf", x_c, w_c)
            d_act = dot32("erd,efd->erf", g_c, w_b)
            kept = gate_c > 0
            act, dh_one, dh_three = [jnp.where(kept, v, 0.0).astype(jnp.bfloat16) for v in swiglu_hidden(h_one, h_three, d_act)]
            dw_two = dot32("erf,erd->efd", act, g_c)
            dw_one = dot32("erd,erf->edf", x_c, dh_one)
            dw_three = dot32("erd,erf->edf", x_c, dh_three)
            grads.append((
                lax.psum_scatter(dw_one, "fsdp", scatter_dimension=1, tiled=True),
                lax.psum_scatter(dw_two, "fsdp", scatter_dimension=2, tiled=True),
                lax.psum_scatter(dw_three, "fsdp", scatter_dimension=1, tiled=True),
            ))
            dx_c = (dot32("erf,edf->erd", dh_one, w_a) + dot32("erf,edf->erd", dh_three, w_c)).astype(jnp.bfloat16)
            dx_chunks.append(dx_c.reshape(per, ep_size, capacity, model_dim))
            y_c = dot32("erf,efd->erd", act, w_b)
            dgate_chunks.append(jnp.sum(dy_c * y_c, axis=-1))

        dx_part = sum_rows(dx_chunks, tokens, tok_dev)
        from_core = swap(dx_part[3], 1)
        to_chip = dx_part[2] + from_core
        from_chip = swap(to_chip, 2)
        dx_near = swap(dx_part[1], 1)

        dgate = jnp.concatenate(dgate_chunks).reshape(n_local, ep_size, capacity).swapaxes(0, 1)
        dgate = jnp.stack([pick(dgate, me ^ k) for k in range(ep_size)])
        dgate = lax.all_to_all(dgate, "ep", 0, 0, tiled=True).reshape(-1)
        dgate_loc = jnp.concatenate([dgate, jnp.zeros((1,), jnp.float32)])[slot_idx].reshape(tok_dev, top_k)

        h_one = dot32("td,df->tf", x_loc, ws_one_full)
        h_three = dot32("td,df->tf", x_loc, ws_three_full)
        d_act = dot32("td,fd->tf", dy_loc, ws_two_full)
        act, dh_one, dh_three = [v.astype(jnp.bfloat16) for v in swiglu_hidden(h_one, h_three, d_act)]
        sff = act.shape[1]
        dx_shared = (dot32("tf,df->td", dh_one, ws_one_full) + dot32("tf,df->td", dh_three, ws_three_full)).astype(jnp.bfloat16)
        shared = jnp.stack([dot32("td,tf->df", x_loc, dh_one), dot32("td,tf->df", dy_loc, act), dot32("td,tf->df", x_loc, dh_three)])
        shared = shared.reshape(3, fs_size, ep_size, model_dim // (fs_size * ep_size), sff)
        by_place = [pick(shared, me ^ m, 2) for m in range(ep_size)]
        near = by_place[0] + swap(by_place[1], 1)
        far = by_place[2] + swap(by_place[3], 1)
        near = near + swap(far, 2)
        mine = pick(near, row, 1) + swap_fs(pick(near, row ^ 1, 1))
        pieces = jnp.stack(spread(mine), axis=1)
        pieces = jnp.stack([pick(pieces, me ^ k, 1) for k in range(ep_size)], axis=1).reshape(3, model_dim // fs_size, sff)

        total = (dx_part[0] + dx_near) + from_chip
        dx_loc = (total.reshape(tok_dev, model_dim) + dx_shared.astype(jnp.float32)).astype(jnp.bfloat16)
        dw_one, dw_two, dw_three = [jnp.concatenate([g[i] for g in grads]) for i in range(3)]
        return dx_loc, dgate_loc, dw_one, dw_two, dw_three, pieces[0], pieces[1].T, pieces[2]

    return jax.shard_map(device_step, mesh=mesh, in_specs=in_specs, out_specs=out_specs, check_vma=False)
```

```python
import jax
import jax.numpy as jnp
from jax import lax
from jax.experimental import pallas as pl
from jax.experimental.pallas import tpu as pltpu
from jax.sharding import PartitionSpec as P

CAP_NUM = 5
CAP_DEN = 4
LANES = 128
UNROLL = 8
CHUNKS = 2


def capacity_for(tok_dev, top_k, n_exp):
    needed = -(-(tok_dev * top_k * CAP_NUM) // (CAP_DEN * n_exp))
    return max(8, -(-needed // 8) * 8)


def route_slots(ids_dev, gate_dev, n_exp, capacity):
    top_k = ids_dev.shape[1]
    flat_ids = ids_dev.reshape(-1)
    n_assign = flat_ids.shape[0]
    onehot = (flat_ids[:, None] == jnp.arange(n_exp, dtype=jnp.int32)[None, :]).astype(jnp.int32)
    slot_pos = jnp.sum(jnp.cumsum(onehot, axis=0) * onehot, axis=1) - 1
    slot_idx = jnp.where(slot_pos < capacity, flat_ids * capacity + slot_pos, n_exp * capacity)
    tokens = jnp.zeros((n_exp * capacity + 1,), jnp.int32).at[slot_idx].set(jnp.arange(n_assign, dtype=jnp.int32) // top_k)
    gates = jnp.zeros((n_exp * capacity + 1,), jnp.float32).at[slot_idx].set(gate_dev.reshape(-1))
    return slot_idx, tokens[: n_exp * capacity], gates[: n_exp * capacity]


def gather_rows(tables, tokens, n_local, capacity):
    n_src = len(tables)
    tok_dev, dim = tables[0].shape
    parts = dim // LANES
    per = n_local // CHUNKS

    def body(tok_ref, *refs):
        tabs, outs = refs[:n_src], refs[n_src : n_src + CHUNKS]
        raw, wide, rows, sem = refs[n_src + CHUNKS :]
        src = pl.program_id(0)
        expert = pl.program_id(1)

        @pl.when(expert == 0)
        def _():
            for m in range(n_src):
                @pl.when(src == m)
                def _():
                    copy = pltpu.make_async_copy(tabs[m], raw, sem)
                    copy.start()
                    copy.wait()

            @pl.loop(0, tok_dev // LANES)
            def _(i):
                base = pl.multiple_of(i * LANES, LANES)
                for j in range(parts):
                    piece = raw[pl.ds(base, LANES), j * LANES : (j + 1) * LANES].astype(jnp.float32)
                    wide[pl.ds(base * parts + j, LANES, stride=parts), :] = piece

        first = expert * capacity

        @pl.loop(0, capacity // UNROLL)
        def _(i):
            for k in range(UNROLL):
                slot = i * UNROLL + k
                tok = pl.multiple_of(tok_ref[0, 0, first + slot] * parts, parts)
                rows[pl.ds(pl.multiple_of(slot * parts, parts), parts), :] = wide[pl.ds(tok, parts), :]

        for c in range(CHUNKS):
            @pl.when(expert // per == c)
            def _():
                for j in range(parts):
                    outs[c][0, 0, :, j * LANES : (j + 1) * LANES] = rows[pl.ds(j, capacity, stride=parts), :].astype(outs[c].dtype)

    def block_of(c):
        return pl.BlockSpec((1, 1, capacity, dim), lambda s, e: (jnp.clip(e - c * per, 0, per - 1), s, 0, 0))

    return pl.pallas_call(
        body,
        grid=(n_src, n_local),
        in_specs=[pl.BlockSpec((1, 1, n_local * capacity), lambda s, e: (s, 0, 0), memory_space=pltpu.SMEM)]
        + [pl.BlockSpec(memory_space=pl.ANY)] * n_src,
        out_specs=[block_of(c) for c in range(CHUNKS)],
        out_shape=[jax.ShapeDtypeStruct((per, n_src, capacity, dim), tables[0].dtype)] * CHUNKS,
        scratch_shapes=[
            pltpu.VMEM((tok_dev, dim), tables[0].dtype),
            pltpu.VMEM((tok_dev * parts, LANES), jnp.float32),
            pltpu.VMEM((capacity * parts, LANES), jnp.float32),
            pltpu.SemaphoreType.DMA,
        ],
        compiler_params=pltpu.CompilerParams(vmem_limit_bytes=40 * 2**20),
        cost_estimate=pl.CostEstimate(flops=600_000_000, bytes_accessed=100_000_000, transcendentals=0),
        name="gather_rows",
    )(tokens.reshape(n_src, 1, n_local * capacity), *tables)


def sum_rows(row_chunks, tokens, source, tok_dev):
    n_chunks = len(row_chunks)
    per_chunk, _, capacity, dim = row_chunks[0].shape
    n_local = per_chunk * n_chunks
    parts = dim // LANES

    def body(tok_ref, *refs):
        chunks, out_ref, wide = refs[:n_chunks], *refs[n_chunks:]
        step = pl.program_id(0)

        @pl.when(step == 0)
        def _():
            @pl.loop(0, tok_dev * parts // 256)
            def _(i):
                out_ref[pl.ds(pl.multiple_of(i * 256, 256), 256), :] = jnp.zeros((256, LANES), jnp.float32)

        for c in range(n_chunks):
            for j in range(parts):
                wide[pl.ds(j, capacity, stride=parts), :] = chunks[c][0, 0, :, j * LANES : (j + 1) * LANES].astype(jnp.float32)
            first = (step + c * per_chunk) * capacity

            @pl.loop(0, capacity // UNROLL)
            def _(i):
                where, sums = [], []
                for k in range(UNROLL):
                    slot = i * UNROLL + k
                    tok = pl.multiple_of(tok_ref[0, first + slot] * parts, parts)
                    where.append(tok)
                    row = wide[pl.ds(pl.multiple_of(slot * parts, parts), parts), :]
                    sums.append(out_ref[pl.ds(tok, parts), :] + row)
                for k in reversed(range(UNROLL)):
                    out_ref[pl.ds(where[k], parts), :] = sums[k]

    return pl.pallas_call(
        body,
        grid=(per_chunk,),
        in_specs=[pl.BlockSpec((1, n_local * capacity), lambda e: (0, 0), memory_space=pltpu.SMEM)]
        + [pl.BlockSpec((1, 1, capacity, dim), lambda e: (e, source, 0, 0))] * n_chunks,
        out_specs=pl.BlockSpec((tok_dev * parts, LANES), lambda e: (0, 0)),
        out_shape=jax.ShapeDtypeStruct((tok_dev * parts, LANES), jnp.float32),
        scratch_shapes=[pltpu.VMEM((capacity * parts, LANES), jnp.float32)],
        compiler_params=pltpu.CompilerParams(vmem_limit_bytes=56 * 2**20),
        cost_estimate=pl.CostEstimate(flops=150_000_000, bytes_accessed=32_000_000, transcendentals=0),
        name="sum_rows",
    )(tokens.reshape(1, n_local * capacity), *row_chunks)


def swiglu_hidden(h_one, h_three, d_act):
    sig_one = jax.nn.sigmoid(h_one)
    silu_one = h_one * sig_one
    return silu_one * h_three, d_act * h_three * sig_one * (1.0 + h_one * (1.0 - sig_one)), d_act * silu_one


def dot32(form, a, b):
    return jnp.einsum(form, a, b, preferred_element_type=jnp.float32)


def solution(mesh):
    ep_size = mesh.shape["ep"]
    fs_size = mesh.shape["fsdp"]
    tok_spec = P(("fsdp", "ep"), None)
    in_specs = (tok_spec, tok_spec, tok_spec, tok_spec, P("ep", "fsdp", None), P("ep", None, "fsdp"), P("ep", "fsdp", None), P("fsdp", None), P(None, "fsdp"), P("fsdp", None))
    out_specs = (tok_spec, tok_spec, P("ep", "fsdp", None), P("ep", None, "fsdp"), P("ep", "fsdp", None), P("fsdp", None), P(None, "fsdp"), P("fsdp", None))

    def swap(value, bit):
        return lax.ppermute(value, "ep", [(i, i ^ bit) for i in range(ep_size)])

    def tie(*values):
        return lax.optimization_barrier(values)

    def swap_fs(value):
        return lax.ppermute(value, "fsdp", [(i, i ^ 1) for i in range(fs_size)])

    def device_step(x_loc, dy_loc, ids_loc, gate_loc, w_one, w_two, w_three, ws_one, ws_two, ws_three):
        tok_dev, top_k = ids_loc.shape
        model_dim = x_loc.shape[1]
        n_local, _, ff = w_one.shape
        n_exp = n_local * ep_size
        capacity = capacity_for(tok_dev, top_k, n_exp)
        me = lax.axis_index("ep")
        row = lax.axis_index("fsdp")
        pick = lambda a, i, axis=0: lax.dynamic_index_in_dim(a, i, axis, keepdims=False)

        def spread(value, near, across):
            return [value, near, across, swap(across, 1)]

        x_near, x_across = swap(x_loc, 1), swap(x_loc, 2)
        dy_near, dy_across = swap(dy_loc, 1), swap(dy_loc, 2)

        slot_idx, slot_tok, slot_gate = route_slots(ids_loc, gate_loc, n_exp, capacity)
        table = jnp.stack([slot_tok.astype(jnp.float32), slot_gate]).reshape(2, ep_size, n_local, capacity).swapaxes(0, 1)
        table, x_across = tie(table, x_across)
        table = lax.all_to_all(table, "ep", 0, 0, tiled=True)
        x_tabs = spread(x_loc, x_near, x_across)
        table = jnp.stack([pick(table, me ^ m) for m in range(ep_size)])
        tokens = table[:, 0].astype(jnp.int32)
        gates = table[:, 1].swapaxes(0, 1).reshape(n_local, ep_size * capacity, 1)

        per = n_local // CHUNKS
        weights = []
        for c in range(CHUNKS):
            part = slice(c * per, (c + 1) * per)
            weights.append((
                lax.all_gather(w_one[part], "fsdp", axis=1, tiled=True),
                lax.all_gather(w_three[part], "fsdp", axis=1, tiled=True),
                lax.all_gather(w_two[part], "fsdp", axis=2, tiled=True),
            ))
        ws_one_full = lax.all_gather(ws_one, "fsdp", axis=0, tiled=True)
        ws_three_full = lax.all_gather(ws_three, "fsdp", axis=0, tiled=True)
        ws_two_full = lax.all_gather(ws_two, "fsdp", axis=1, tiled=True)

        x_rows = [r.reshape(per, ep_size * capacity, model_dim) for r in gather_rows(x_tabs, tokens, n_local, capacity)]
        x_rows[0], dy_across = tie(x_rows[0], dy_across)
        dy_tabs = spread(dy_loc, dy_near, dy_across)
        dy_rows = [r.reshape(per, ep_size * capacity, model_dim) for r in gather_rows(dy_tabs, tokens, n_local, capacity)]

        dx_chunks, acts, grads = [], [], []
        for c in range(CHUNKS):
            part = slice(c * per, (c + 1) * per)
            w_a, w_c, w_b = weights[c]
            x_c, dy_c, gate_c = x_rows[c], dy_rows[c], gates[part]
            g_c = (gate_c * dy_c.astype(jnp.float32)).astype(jnp.bfloat16)
            h_one = dot32("erd,edf->erf", x_c, w_a)
            h_three = dot32("erd,edf->erf", x_c, w_c)
            d_act = dot32("erd,efd->erf", g_c, w_b)
            kept = gate_c > 0
            act, dh_one, dh_three = [jnp.where(kept, v, 0.0).astype(jnp.bfloat16) for v in swiglu_hidden(h_one, h_three, d_act)]
            dw_two = dot32("erf,erd->efd", act, g_c)
            dw_one = dot32("erd,erf->edf", x_c, dh_one)
            dw_three = dot32("erd,erf->edf", x_c, dh_three)
            dx_c = (dot32("erf,edf->erd", dh_one, w_a) + dot32("erf,edf->erd", dh_three, w_c)).astype(jnp.bfloat16)
            if c + 1 < CHUNKS:
                x_rows[c + 1], dy_rows[c + 1], dw_one, dw_two, dw_three, dx_c = tie(x_rows[c + 1], dy_rows[c + 1], dw_one, dw_two, dw_three, dx_c)
            grads.append((
                lax.psum_scatter(dw_one, "fsdp", scatter_dimension=1, tiled=True),
                lax.psum_scatter(dw_two, "fsdp", scatter_dimension=2, tiled=True),
                lax.psum_scatter(dw_three, "fsdp", scatter_dimension=1, tiled=True),
            ))
            dx_chunks.append(dx_c.reshape(per, ep_size, capacity, model_dim))
            acts.append(act)

        dx_part = {m: sum_rows(dx_chunks, tokens[m], m, tok_dev) for m in (3, 1, 2, 0)}
        from_core = swap(dx_part[3], 1)
        dx_near = swap(dx_part[1], 1)
        dx_part[0], x_loc, dy_loc, *acts = tie(dx_part[0], x_loc, dy_loc, *acts)
        to_chip = dx_part[2] + from_core
        from_chip = swap(to_chip, 2)

        dgate_chunks = [
            jnp.sum(acts[c].astype(jnp.float32) * dot32("erd,efd->erf", dy_rows[c], weights[c][2]), axis=-1)
            for c in range(CHUNKS)
        ]
        dgate = jnp.concatenate(dgate_chunks).reshape(n_local, ep_size, capacity).swapaxes(0, 1)
        dgate = jnp.stack([pick(dgate, me ^ k) for k in range(ep_size)])
        dgate = lax.all_to_all(dgate, "ep", 0, 0, tiled=True).reshape(-1)
        dgate_loc = jnp.concatenate([dgate, jnp.zeros((1,), jnp.float32)])[slot_idx].reshape(tok_dev, top_k)

        h_one = dot32("td,df->tf", x_loc, ws_one_full)
        h_three = dot32("td,df->tf", x_loc, ws_three_full)
        d_act = dot32("td,fd->tf", dy_loc, ws_two_full)
        act, dh_one, dh_three = [v.astype(jnp.bfloat16) for v in swiglu_hidden(h_one, h_three, d_act)]
        sff = act.shape[1]
        dx_shared = (dot32("tf,df->td", dh_one, ws_one_full) + dot32("tf,df->td", dh_three, ws_three_full)).astype(jnp.bfloat16)
        shared = jnp.stack([dot32("td,tf->df", x_loc, dh_one), dot32("td,tf->df", dy_loc, act), dot32("td,tf->df", x_loc, dh_three)])
        shared = shared.reshape(3, fs_size, ep_size, model_dim // (fs_size * ep_size), sff)
        by_place = [pick(shared, me ^ m, 2) for m in range(ep_size)]
        near = by_place[0] + swap(by_place[1], 1)
        far = by_place[2] + swap(by_place[3], 1)
        near = near + swap(far, 2)
        mine = pick(near, row, 1) + swap_fs(pick(near, row ^ 1, 1))
        pieces = jnp.stack(spread(mine, swap(mine, 1), swap(mine, 2)), axis=1)
        pieces = jnp.stack([pick(pieces, me ^ k, 1) for k in range(ep_size)], axis=1).reshape(3, model_dim // fs_size, sff)

        total = (dx_part[0] + dx_near) + from_chip
        dx_loc = (total.reshape(tok_dev, model_dim) + dx_shared.astype(jnp.float32)).astype(jnp.bfloat16)
        dw_one, dw_two, dw_three = [jnp.zeros((n_local,) + grads[0][i].shape[1:], jnp.float32) for i in range(3)]
        for c in range(CHUNKS):
            dw_one, dw_two, dw_three = [lax.dynamic_update_slice(a, g, (c * per, 0, 0)) for a, g in zip((dw_one, dw_two, dw_three), grads[c])]
        return dx_loc, dgate_loc, dw_one, dw_two, dw_three, pieces[0], pieces[1].T, pieces[2]

    return jax.shard_map(device_step, mesh=mesh, in_specs=in_specs, out_specs=out_specs, check_vma=False)
```

```python
import jax
import jax.numpy as jnp
from jax import lax
from jax.experimental import pallas as pl
from jax.experimental.pallas import tpu as pltpu
from jax.sharding import PartitionSpec as P

CAP_NUM = 5
CAP_DEN = 4
LANES = 128
UNROLL = 8
CHUNKS = 2


def capacity_for(tok_dev, top_k, n_exp):
    needed = -(-(tok_dev * top_k * CAP_NUM) // (CAP_DEN * n_exp))
    return max(8, -(-needed // 8) * 8)


def route_slots(ids_dev, gate_dev, n_exp, capacity):
    top_k = ids_dev.shape[1]
    flat_ids = ids_dev.reshape(-1)
    n_assign = flat_ids.shape[0]
    onehot = (flat_ids[:, None] == jnp.arange(n_exp, dtype=jnp.int32)[None, :]).astype(jnp.int32)
    slot_pos = jnp.sum(jnp.cumsum(onehot, axis=0) * onehot, axis=1) - 1
    slot_idx = jnp.where(slot_pos < capacity, flat_ids * capacity + slot_pos, n_exp * capacity)
    tokens = jnp.zeros((n_exp * capacity + 1,), jnp.int32).at[slot_idx].set(jnp.arange(n_assign, dtype=jnp.int32) // top_k)
    gates = jnp.zeros((n_exp * capacity + 1,), jnp.float32).at[slot_idx].set(gate_dev.reshape(-1))
    return slot_idx, tokens[: n_exp * capacity], gates[: n_exp * capacity]


def gather_rows(tables, tokens, n_local, capacity):
    n_src = len(tables)
    tok_dev, dim = tables[0].shape
    parts = dim // LANES
    per = n_local // CHUNKS

    def body(tok_ref, *refs):
        tabs, outs = refs[:n_src], refs[n_src : n_src + CHUNKS]
        raw, wide, rows, sem = refs[n_src + CHUNKS :]
        src = pl.program_id(0)
        expert = pl.program_id(1)

        @pl.when(expert == 0)
        def _():
            for m in range(n_src):
                @pl.when(src == m)
                def _():
                    copy = pltpu.make_async_copy(tabs[m], raw, sem)
                    copy.start()
                    copy.wait()

            @pl.loop(0, tok_dev // LANES)
            def _(i):
                base = pl.multiple_of(i * LANES, LANES)
                for j in range(parts):
                    piece = raw[pl.ds(base, LANES), j * LANES : (j + 1) * LANES].astype(jnp.float32)
                    wide[pl.ds(base * parts + j, LANES, stride=parts), :] = piece

        first = expert * capacity

        @pl.loop(0, capacity // UNROLL)
        def _(i):
            for k in range(UNROLL):
                slot = i * UNROLL + k
                tok = pl.multiple_of(tok_ref[0, 0, first + slot] * parts, parts)
                rows[pl.ds(pl.multiple_of(slot * parts, parts), parts), :] = wide[pl.ds(tok, parts), :]

        for c in range(CHUNKS):
            @pl.when(expert // per == c)
            def _():
                for j in range(parts):
                    outs[c][0, 0, :, j * LANES : (j + 1) * LANES] = rows[pl.ds(j, capacity, stride=parts), :].astype(outs[c].dtype)

    def block_of(c):
        return pl.BlockSpec((1, 1, capacity, dim), lambda s, e: (jnp.clip(e - c * per, 0, per - 1), s, 0, 0))

    return pl.pallas_call(
        body,
        grid=(n_src, n_local),
        in_specs=[pl.BlockSpec((1, 1, n_local * capacity), lambda s, e: (s, 0, 0), memory_space=pltpu.SMEM)]
        + [pl.BlockSpec(memory_space=pl.ANY)] * n_src,
        out_specs=[block_of(c) for c in range(CHUNKS)],
        out_shape=[jax.ShapeDtypeStruct((per, n_src, capacity, dim), tables[0].dtype)] * CHUNKS,
        scratch_shapes=[
            pltpu.VMEM((tok_dev, dim), tables[0].dtype),
            pltpu.VMEM((tok_dev * parts, LANES), jnp.float32),
            pltpu.VMEM((capacity * parts, LANES), jnp.float32),
            pltpu.SemaphoreType.DMA,
        ],
        compiler_params=pltpu.CompilerParams(vmem_limit_bytes=40 * 2**20),
        cost_estimate=pl.CostEstimate(flops=600_000_000, bytes_accessed=100_000_000, transcendentals=0),
        name="gather_rows",
    )(tokens.reshape(n_src, 1, n_local * capacity), *tables)


def sum_rows(row_chunks, tokens, source, tok_dev):
    n_chunks = len(row_chunks)
    per_chunk, _, capacity, dim = row_chunks[0].shape
    n_local = per_chunk * n_chunks
    parts = dim // LANES

    def body(tok_ref, *refs):
        chunks, out_ref, wide = refs[:n_chunks], *refs[n_chunks:]
        step = pl.program_id(0)

        @pl.when(step == 0)
        def _():
            @pl.loop(0, tok_dev * parts // 256)
            def _(i):
                out_ref[pl.ds(pl.multiple_of(i * 256, 256), 256), :] = jnp.zeros((256, LANES), jnp.float32)

        for c in range(n_chunks):
            for j in range(parts):
                wide[pl.ds(j, capacity, stride=parts), :] = chunks[c][0, 0, :, j * LANES : (j + 1) * LANES].astype(jnp.float32)
            first = (step + c * per_chunk) * capacity

            @pl.loop(0, capacity // UNROLL)
            def _(i):
                where, sums = [], []
                for k in range(UNROLL):
                    slot = i * UNROLL + k
                    tok = pl.multiple_of(tok_ref[0, first + slot] * parts, parts)
                    where.append(tok)
                    row = wide[pl.ds(pl.multiple_of(slot * parts, parts), parts), :]
                    sums.append(out_ref[pl.ds(tok, parts), :] + row)
                for k in reversed(range(UNROLL)):
                    out_ref[pl.ds(where[k], parts), :] = sums[k]

    return pl.pallas_call(
        body,
        grid=(per_chunk,),
        in_specs=[pl.BlockSpec((1, n_local * capacity), lambda e: (0, 0), memory_space=pltpu.SMEM)]
        + [pl.BlockSpec((1, 1, capacity, dim), lambda e: (e, source, 0, 0))] * n_chunks,
        out_specs=pl.BlockSpec((tok_dev * parts, LANES), lambda e: (0, 0)),
        out_shape=jax.ShapeDtypeStruct((tok_dev * parts, LANES), jnp.float32),
        scratch_shapes=[pltpu.VMEM((capacity * parts, LANES), jnp.float32)],
        compiler_params=pltpu.CompilerParams(vmem_limit_bytes=56 * 2**20),
        cost_estimate=pl.CostEstimate(flops=150_000_000, bytes_accessed=32_000_000, transcendentals=0),
        name="sum_rows",
    )(tokens.reshape(1, n_local * capacity), *row_chunks)


def swiglu_hidden(h_one, h_three, d_act):
    sig_one = jax.nn.sigmoid(h_one)
    silu_one = h_one * sig_one
    return silu_one * h_three, d_act * h_three * sig_one * (1.0 + h_one * (1.0 - sig_one)), d_act * silu_one


def dot32(form, a, b):
    return jnp.einsum(form, a, b, preferred_element_type=jnp.float32)


def solution(mesh):
    ep_size = mesh.shape["ep"]
    fs_size = mesh.shape["fsdp"]
    tok_spec = P(("fsdp", "ep"), None)
    in_specs = (tok_spec, tok_spec, tok_spec, tok_spec, P("ep", "fsdp", None), P("ep", None, "fsdp"), P("ep", "fsdp", None), P("fsdp", None), P(None, "fsdp"), P("fsdp", None))
    out_specs = (tok_spec, tok_spec, P("ep", "fsdp", None), P("ep", None, "fsdp"), P("ep", "fsdp", None), P("fsdp", None), P(None, "fsdp"), P("fsdp", None))

    def swap(value, bit):
        return lax.ppermute(value, "ep", [(i, i ^ bit) for i in range(ep_size)])

    def tie(*values):
        return lax.optimization_barrier(values)

    def swap_fs(value):
        return lax.ppermute(value, "fsdp", [(i, i ^ 1) for i in range(fs_size)])

    def device_step(x_loc, dy_loc, ids_loc, gate_loc, w_one, w_two, w_three, ws_one, ws_two, ws_three):
        tok_dev, top_k = ids_loc.shape
        model_dim = x_loc.shape[1]
        n_local, _, ff = w_one.shape
        n_exp = n_local * ep_size
        capacity = capacity_for(tok_dev, top_k, n_exp)
        me = lax.axis_index("ep")
        row = lax.axis_index("fsdp")
        pick = lambda a, i, axis=0: lax.dynamic_index_in_dim(a, i, axis, keepdims=False)

        def spread(value, near, across):
            return [value, near, across, swap(across, 1)]

        x_near, x_across = swap(x_loc, 1), swap(x_loc, 2)
        dy_near, dy_across = swap(dy_loc, 1), swap(dy_loc, 2)

        slot_idx, slot_tok, slot_gate = route_slots(ids_loc, gate_loc, n_exp, capacity)
        table = jnp.stack([slot_tok.astype(jnp.float32), slot_gate]).reshape(2, ep_size, n_local, capacity).swapaxes(0, 1)
        table, x_across = tie(table, x_across)
        table = lax.all_to_all(table, "ep", 0, 0, tiled=True)
        x_tabs = spread(x_loc, x_near, x_across)
        table = jnp.stack([pick(table, me ^ m) for m in range(ep_size)])
        tokens = table[:, 0].astype(jnp.int32)
        gates = table[:, 1].swapaxes(0, 1).reshape(n_local, ep_size * capacity, 1)

        per = n_local // CHUNKS
        weights = []
        for c in range(CHUNKS):
            part = slice(c * per, (c + 1) * per)
            weights.append((
                lax.all_gather(w_one[part], "fsdp", axis=1, tiled=True),
                lax.all_gather(w_three[part], "fsdp", axis=1, tiled=True),
                lax.all_gather(w_two[part], "fsdp", axis=2, tiled=True),
            ))
        ws_one_full = lax.all_gather(ws_one, "fsdp", axis=0, tiled=True)
        ws_three_full = lax.all_gather(ws_three, "fsdp", axis=0, tiled=True)
        ws_two_full = lax.all_gather(ws_two, "fsdp", axis=1, tiled=True)

        x_rows = [r.reshape(per, ep_size * capacity, model_dim) for r in gather_rows(x_tabs, tokens, n_local, capacity)]
        x_rows[0], dy_across = tie(x_rows[0], dy_across)
        dy_tabs = spread(dy_loc, dy_near, dy_across)
        dy_rows = [r.reshape(per, ep_size * capacity, model_dim) for r in gather_rows(dy_tabs, tokens, n_local, capacity)]

        dx_chunks, acts, grads = [], [], []
        for c in range(CHUNKS):
            part = slice(c * per, (c + 1) * per)
            w_a, w_c, w_b = weights[c]
            x_c, dy_c, gate_c = x_rows[c], dy_rows[c], gates[part]
            g_c = (gate_c * dy_c.astype(jnp.float32)).astype(jnp.bfloat16)
            h_one = dot32("erd,edf->erf", x_c, w_a)
            h_three = dot32("erd,edf->erf", x_c, w_c)
            d_act = dot32("erd,efd->erf", g_c, w_b)
            kept = gate_c > 0
            act, dh_one, dh_three = [jnp.where(kept, v, 0.0).astype(jnp.bfloat16) for v in swiglu_hidden(h_one, h_three, d_act)]
            dw_two = dot32("erf,erd->efd", act, g_c)
            dw_one = dot32("erd,erf->edf", x_c, dh_one)
            dw_three = dot32("erd,erf->edf", x_c, dh_three)
            dx_c = (dot32("erf,edf->erd", dh_one, w_a) + dot32("erf,edf->erd", dh_three, w_c)).astype(jnp.bfloat16)
            if c + 1 < CHUNKS:
                x_rows[c + 1], dy_rows[c + 1], dx_c = tie(x_rows[c + 1], dy_rows[c + 1], dx_c)
            grads.append((
                lax.psum_scatter(dw_one, "fsdp", scatter_dimension=1, tiled=True),
                lax.psum_scatter(dw_two, "fsdp", scatter_dimension=2, tiled=True),
                lax.psum_scatter(dw_three, "fsdp", scatter_dimension=1, tiled=True),
            ))
            dx_chunks.append(dx_c.reshape(per, ep_size, capacity, model_dim))
            acts.append(act)

        dx_part = {m: sum_rows(dx_chunks, tokens[m], m, tok_dev) for m in (3, 1, 2, 0)}
        from_core = swap(dx_part[3], 1)
        dx_near = swap(dx_part[1], 1)
        dx_part[0], x_loc, dy_loc, *acts = tie(dx_part[0], x_loc, dy_loc, *acts)
        to_chip = dx_part[2] + from_core
        from_chip = swap(to_chip, 2)

        dgate_chunks = [
            jnp.sum(acts[c].astype(jnp.float32) * dot32("erd,efd->erf", dy_rows[c], weights[c][2]), axis=-1)
            for c in range(CHUNKS)
        ]
        dgate = jnp.concatenate(dgate_chunks).reshape(n_local, ep_size, capacity).swapaxes(0, 1)
        dgate = jnp.stack([pick(dgate, me ^ k) for k in range(ep_size)])
        dgate = lax.all_to_all(dgate, "ep", 0, 0, tiled=True).reshape(-1)
        dgate_loc = jnp.concatenate([dgate, jnp.zeros((1,), jnp.float32)])[slot_idx].reshape(tok_dev, top_k)

        h_one = dot32("td,df->tf", x_loc, ws_one_full)
        h_three = dot32("td,df->tf", x_loc, ws_three_full)
        d_act = dot32("td,fd->tf", dy_loc, ws_two_full)
        act, dh_one, dh_three = [v.astype(jnp.bfloat16) for v in swiglu_hidden(h_one, h_three, d_act)]
        sff = act.shape[1]
        dx_shared = (dot32("tf,df->td", dh_one, ws_one_full) + dot32("tf,df->td", dh_three, ws_three_full)).astype(jnp.bfloat16)
        shared = jnp.stack([dot32("td,tf->df", x_loc, dh_one), dot32("td,tf->df", dy_loc, act), dot32("td,tf->df", x_loc, dh_three)])
        shared = shared.reshape(3, fs_size, ep_size, model_dim // (fs_size * ep_size), sff)
        by_place = [pick(shared, me ^ m, 2) for m in range(ep_size)]
        near = by_place[0] + swap(by_place[1], 1)
        far = by_place[2] + swap(by_place[3], 1)
        near = near + swap(far, 2)
        mine = pick(near, row, 1) + swap_fs(pick(near, row ^ 1, 1))
        pieces = jnp.stack(spread(mine, swap(mine, 1), swap(mine, 2)), axis=1)
        pieces = jnp.stack([pick(pieces, me ^ k, 1) for k in range(ep_size)], axis=1).reshape(3, model_dim // fs_size, sff)

        total = (dx_part[0] + dx_near) + from_chip
        dx_loc = (total.reshape(tok_dev, model_dim) + dx_shared.astype(jnp.float32)).astype(jnp.bfloat16)
        dw_one, dw_two, dw_three = [jnp.zeros((n_local,) + grads[0][i].shape[1:], jnp.float32) for i in range(3)]
        for c in range(CHUNKS):
            dw_one, dw_two, dw_three = [lax.dynamic_update_slice(a, g, (c * per, 0, 0)) for a, g in zip((dw_one, dw_two, dw_three), grads[c])]
        return dx_loc, dgate_loc, dw_one, dw_two, dw_three, pieces[0], pieces[1].T, pieces[2]

    return jax.shard_map(device_step, mesh=mesh, in_specs=in_specs, out_specs=out_specs, check_vma=False)
```
